32 devices in a mesh: dp: 4 (over y, x), sp: 4 (over z), shift: 2 (over core).
Axes of the slice: x: 2, y: 2, z: 4, core: 2. Of those that a mesh axis runs over, the one named last changes fastest.
Arguments:
- query_rows: bfloat16 [8, 1024, 32, 128], P(('shift', 'dp'), 'sp'), parts along dimension 0, may hold values from -6 to 6
- key_rows: bfloat16 [8, 1024, 32, 128], P(('shift', 'dp'), 'sp'), parts along dimension 0, may hold values from -6 to 6
- value_rows: bfloat16 [8, 1024, 32, 128], P(('shift', 'dp'), 'sp'), parts along dimension 0, may hold values from -6 to 6
- out_weight: bfloat16 [8192, 4096], P(('shift', 'dp')), parts along dimension 0, may hold values from -0.09375 to 0.09375
Outputs:
- mixer_out: bfloat16 [8, 1024, 4096], P(('shift', 'dp'), 'sp'), parts along dimension 0
The draws below stay inside these ranges and needn't reach their ends.
There are 2 independent parts, one for each index of `shift`. The reference program is written for one: setup_inputs(seed, part) draws one part's arguments, and reference() takes and returns one part's arrays. A program takes and returns all parts, laid end to end along the dimension named above; each array names one. Nothing has to cross between parts.
All inputs are finite; a program needn't handle non-finite values.
Results may differ from the reference program's by a relative error of at most 0.006.
Values may be sent and summed in bfloat16 or wider, within the bound.
No kernel may reach another device: no remote copies, remote signals or barrier semaphores. Data moves between devices by JAX's collectives and lax.ppermute only.
A program may use at most 128 MiB of HBM per device.

```python
import jax
import jax.numpy as jnp
from jax import lax

HEADS = 32
HEAD_SIZE = 128
BATCH = 4
TOKENS = 1024
WIDTH = 4096


def steps_of(key, shape, shards, least, top_value):
    factor_of = 1.0
    for dim, shards_of in shards:
        steps = jax.random.uniform(jax.random.fold_in(jax.random.fold_in(key, 6), dim), (shards_of,), jnp.float32, least / len(shards), top_value / len(shards))
        factor_of = factor_of * jnp.repeat(jnp.exp(steps), shape[dim] // shards_of).reshape((-1,) + (1,) * (len(shape) - 1 - dim))
    return factor_of


def noise(key, dims, scale, most, cuts=(), dtype=jnp.bfloat16):
    entries = jax.random.normal(key, dims, jnp.float32) * scale
    if len(cuts) > 0:
        entries = steps_of(key, dims, cuts, -0.22, 0.18) * entries
    return jnp.clip(entries, min=-most, max=most).astype(dtype)


def setup_inputs(seed: int = 0, part: int = 0) -> dict:
    key_of = jax.random.split(jax.random.key(seed), 5)
    own_keys = jax.random.split(jax.random.fold_in(key_of[4], part), 5)
    return {
        "query_rows": noise(own_keys[0], (BATCH, TOKENS, HEADS, HEAD_SIZE), 1.0, 6.0, ((0, 4), (1, 4))),
        "key_rows": noise(own_keys[1], (BATCH, TOKENS, HEADS, HEAD_SIZE), 1.0, 6.0, ((0, 4), (1, 4))),
        "value_rows": noise(own_keys[2], (BATCH, TOKENS, HEADS, HEAD_SIZE), 1.0, 6.0, ((0, 4), (1, 4))),
        "out_weight": noise(own_keys[3], (WIDTH, WIDTH), WIDTH ** -0.5, 0.09375, ((0, 4),)),
    }


def feature_map(values):
    wide = values.astype(jnp.float32)
    return (jnp.where(wide > 0.0, wide + 1.0, jnp.exp(jnp.minimum(wide, 0.0)))).astype(jnp.bfloat16)


def finish_heads(read, count):
    result = read * count ** 0.5
    return result.astype(jnp.bfloat16)


def ask_state(features, state, mass):
    small = lax.optimization_barrier(state.astype(jnp.bfloat16))
    top = jnp.einsum("bthd,bhde->bthe", features.astype(jnp.float32), small.astype(jnp.float32))
    bottom = jnp.einsum("bthd,bhd->bth", features.astype(jnp.float32), mass, precision=lax.Precision.HIGHEST)
    return top / (bottom + 1e-3)[..., None]


def reference(query_rows, key_rows, value_rows, out_weight):
    query_feature, key_feature = lax.optimization_barrier((feature_map(query_rows), feature_map(key_rows)))
    state = jnp.einsum("bthd,bthe->bhde", key_feature.astype(jnp.float32), value_rows.astype(jnp.float32)) / TOKENS
    mass = jnp.sum(key_feature.astype(jnp.float32), axis=1) / TOKENS
    mixed = finish_heads(ask_state(query_feature, state, mass), TOKENS).reshape(BATCH, TOKENS, WIDTH)
    mixed = lax.optimization_barrier(mixed)
    mixer_out = jnp.einsum("btw,wv->btv", mixed.astype(jnp.float32), out_weight.astype(jnp.float32)).astype(jnp.bfloat16)
    return mixer_out
```

```python
import functools
import math

import jax
import jax.numpy as jnp
from jax import lax
from jax.experimental import pallas as pl
from jax.experimental.pallas import tpu as pltpu
from jax.sharding import PartitionSpec as P

F32, BF16 = jnp.float32, jnp.bfloat16
CHUNKS = 2


def ring_order(n):
    side = math.isqrt(n)
    if side * side != n or side % 2:
        return list(range(n))
    order = list(range(side))
    for row in range(1, side):
        cols = range(1, side)
        order += [row * side + c for c in (reversed(cols) if row % 2 else cols)]
    order += [row * side for row in range(side - 1, 0, -1)]
    return order


def feature_map(values):
    wide = values.astype(F32)
    return jnp.where(wide > 0.0, wide + 1.0, jnp.exp(jnp.minimum(wide, 0.0))).astype(BF16)


def cost(flops, nbytes):
    return pl.CostEstimate(flops=flops, bytes_accessed=nbytes, transcendentals=0)


def split_mass(mass):
    high = mass.astype(BF16)
    low = (mass - high.astype(F32)).astype(BF16)
    return jnp.concatenate([high, low], axis=0)


def state_kernel(parts, index, key, value, *refs):
    outs, (keys, values, states) = refs[:parts], refs[parts:]
    tokens, heads, size = key.shape[1:]
    rows = heads * size // parts
    feature = feature_map(key[0]).astype(F32)
    mass = split_mass(jnp.sum(feature, axis=0))
    keys[...] = feature.reshape(tokens * heads, size)
    values[...] = value[0].astype(F32).reshape(tokens * heads, size)
    for h in range(heads):
        states[h * size : (h + 1) * size, :] = lax.dot_general(
            keys[pl.ds(h, tokens, stride=heads), :].astype(BF16),
            values[pl.ds(h, tokens, stride=heads), :].astype(BF16),
            (((0,), (0,)), ((), ())),
            preferred_element_type=F32,
        )
    place = index[index.shape[0] - 1]
    for j in range(parts):
        start = pl.multiple_of(lax.rem(place + j, parts) * rows, rows)
        outs[j][0, :rows, :] = states[pl.ds(start, rows), :].astype(BF16)
        outs[j][0, rows:, :] = mass


def partial_states(key, value, index, blocks, heads, parts):
    _, tokens, _, size = key.shape
    rows = heads * size // parts + 2 * heads
    block = pl.BlockSpec((1, tokens, heads, size), lambda i, s: (0, 0, s[i], 0))
    return pl.pallas_call(
        functools.partial(state_kernel, parts),
        grid_spec=pltpu.PrefetchScalarGridSpec(
            num_scalar_prefetch=1,
            grid=(blocks,),
            in_specs=[block, block],
            out_specs=[pl.BlockSpec((1, rows, size), lambda i, s: (i, 0, 0))] * parts,
            scratch_shapes=[
                pltpu.VMEM((tokens * heads, size), F32),
                pltpu.VMEM((tokens * heads, size), F32),
                pltpu.VMEM((heads * size, size), F32),
            ],
        ),
        out_shape=[jax.ShapeDtypeStruct((blocks, rows, size), BF16)] * parts,
        cost_estimate=cost(blocks * heads * tokens * size * size * 2, blocks * heads * tokens * size * 4),
        name="partial_states",
    )(index, key, value)


def total_kernel(blocks, heads, count, *refs):
    takes, outs = refs[:-blocks], refs[-blocks:]
    rows = takes[0].shape[1] - 2 * heads
    for b in range(blocks):
        total = takes[0][b].astype(F32)
        for take in takes[1:]:
            total = total + take[b].astype(F32)
        total = total / count
        outs[b][:rows, :] = total[:rows].astype(BF16)
        mass = total[rows : rows + heads] + total[rows + heads :]
        outs[b][rows:, :] = split_mass(mass)


def total_states(takes, heads, count):
    blocks, rows, size = takes[0].shape
    return pl.pallas_call(
        functools.partial(total_kernel, blocks, heads, count),
        out_shape=[jax.ShapeDtypeStruct((rows, size), BF16)] * blocks,
        cost_estimate=cost(blocks * rows * size * 8, blocks * rows * size * 10),
        name="total_states",
    )(*takes)


def read_kernel(parts, scale, place, query, mass, *refs):
    pieces, (out, queries, states) = refs[:parts], refs[parts:]
    tokens, heads, size = query.shape[1:]
    rows = pieces[0].shape[1]
    for j in range(parts):
        start = pl.multiple_of(lax.rem(place[0] + parts - j, parts) * rows, rows)
        states[pl.ds(start, rows), :] = pieces[j][0]
    queries[...] = feature_map(query[0]).astype(F32).reshape(tokens * heads, size)
    masses = mass[...].astype(F32)
    across = (((1,), (1,)), ((), ()))
    for h in range(heads):
        feature = queries[pl.ds(h, tokens, stride=heads), :].astype(BF16)
        top = jnp.dot(feature, states[h * size : (h + 1) * size, :], preferred_element_type=F32)
        bottom = 0.0
        for r in (h, heads + h):
            row = jnp.broadcast_to(masses[r : r + 1, :], (size, size)).astype(BF16)
            bottom += lax.dot_general(feature, row, across, preferred_element_type=F32)
        out[:, h * size : (h + 1) * size] = (top / (bottom + 0.001) * scale).astype(BF16)


def read_states(query, mass, pieces, slot, place, scale):
    parts = len(pieces)
    _, tokens, heads, size = query.shape
    rows = pieces[0].shape[1]
    return pl.pallas_call(
        functools.partial(read_kernel, parts, scale),
        grid_spec=pltpu.PrefetchScalarGridSpec(
            num_scalar_prefetch=1,
            grid=(1,),
            in_specs=[
                pl.BlockSpec((1, tokens, heads, size), lambda i, s: (0, 0, 0, 0)),
                pl.BlockSpec((2 * heads, size), lambda i, s: (0, 0)),
            ]
            + [pl.BlockSpec((1, rows, size), lambda i, s: (slot, 0, 0))] * parts,
            out_specs=pl.BlockSpec((tokens, heads * size), lambda i, s: (0, 0)),
            scratch_shapes=[
                pltpu.VMEM((tokens * heads, size), F32),
                pltpu.VMEM((heads * size, size), BF16),
            ],
        ),
        out_shape=jax.ShapeDtypeStruct((tokens, heads * size), BF16),
        cost_estimate=cost(heads * tokens * size * size * 6, heads * tokens * size * 4),
        name="read_states",
    )(place, query, mass, *pieces)


def partial_states_plain(key, value, index, blocks, heads, parts):
    _, tokens, _, size = key.shape
    outs = [[] for _ in range(parts)]
    for b in range(blocks):
        key_block = feature_map(lax.dynamic_slice_in_dim(key[0], index[b] * heads, heads, 1))
        value_block = lax.dynamic_slice_in_dim(value[0], index[b] * heads, heads, 1)
        state = jnp.einsum("thd,the->hde", key_block, value_block, preferred_element_type=F32)
        state = state.reshape(heads * size, size).astype(BF16)
        mass = split_mass(jnp.sum(key_block.astype(F32), axis=0))
        rows = heads * size // parts
        for j in range(parts):
            start = lax.rem(index[blocks] + j, parts) * rows
            piece = lax.dynamic_slice_in_dim(state, start, rows, 0)
            outs[j].append(jnp.concatenate([piece, mass]))
    return [jnp.stack(out) for out in outs]


def total_states_plain(takes, heads, count):
    total = sum(take.astype(F32) for take in takes) / count
    rows = total.shape[1] - 2 * heads
    mass = total[:, rows : rows + heads] + total[:, rows + heads :]
    return [
        jnp.concatenate([total[b, :rows].astype(BF16), split_mass(mass[b])])
        for b in range(total.shape[0])
    ]


def read_states_plain(query, mass, pieces, slot, place, scale):
    parts = len(pieces)
    _, tokens, heads, size = query.shape
    stack = jnp.stack([piece[slot] for piece in pieces])
    order = lax.rem(place[0] + parts - jnp.arange(parts), parts)
    state = stack[order].reshape(heads, size, size)
    feature = feature_map(query[0])
    whole = mass[:heads].astype(F32) + mass[heads:].astype(F32)
    top = jnp.einsum("thd,hde->the", feature, state, preferred_element_type=F32)
    bottom = jnp.einsum(
        "thd,hd->th", feature.astype(F32), whole, precision=lax.Precision.HIGHEST
    )
    read = top / (bottom + 0.001)[..., None] * scale
    return read.astype(BF16).reshape(tokens, heads * size)


def body(query_rows, key_rows, value_rows, out_weight):
    n, parts = lax.axis_size("dp"), lax.axis_size("sp")
    _, tokens, all_heads, size = query_rows.shape
    heads, width = all_heads // n, out_weight.shape[1]
    count = tokens * parts
    fits = heads % 8 == 0 and (heads * size) % (16 * parts) == 0
    make_partial = partial_states if fits else partial_states_plain
    make_total = total_states if fits else total_states_plain
    make_read = read_states if fits else read_states_plain

    ring = ring_order(n)
    to = [[ring[(ring.index(d) + o) % n] for o in range(n)] for d in range(n)]
    place = lax.axis_index("sp")
    block_of = jnp.array(to, jnp.int32)[lax.axis_index("dp")]

    def around(x, offset):
        return lax.ppermute(x, "dp", [(d, to[d][offset % n]) for d in range(n)])

    def along(x, offset):
        return lax.ppermute(x, "sp", [(i, (i + offset) % parts) for i in range(parts)])

    offsets = [1, n - 1] + list(range(2, n - 1)) + [0]
    if n < 3:
        offsets = list(range(1, n)) + [0]
    index = jnp.concatenate([jnp.stack([block_of[o] for o in offsets]), place[None]])
    sent = make_partial(key_rows, value_rows, index, n, heads, parts)
    queries = {}
    for o in offsets:
        piece = lax.dynamic_slice_in_dim(query_rows, block_of[o] * heads, heads, 2)
        queries[-o % n] = around(piece, o) if o else piece

    takes = [sent[0]] + [along(sent[j], j) for j in range(1, parts)]
    totals = make_total(takes, heads, count)
    own = {-o % n: around(totals[i], o) if o else totals[i] for i, o in enumerate(offsets)}
    slots = [-o % n for o in offsets]
    stack = jnp.stack([own[s][: -2 * heads] for s in slots])
    pieces = [stack] + [along(stack, j) for j in range(1, parts)]
    mixed = {
        s: make_read(queries[s], own[s][-2 * heads :], pieces, i, place[None], count**0.5)
        for i, s in enumerate(slots)
    }

    lanes = []
    step = width // (2 * CHUNKS)
    for c in range(2 * CHUNKS):
        way = 1 if c % 2 == 0 else -1
        lanes.append((way, out_weight[:, c * step : (c + 1) * step]))
    accs = [
        jnp.dot(mixed[-way % n], weight, preferred_element_type=F32).astype(BF16)
        for way, weight in lanes
    ]
    for k in range(1, n):
        accs = [
            (
                jnp.dot(mixed[-way * (k + 1) % n], weight, preferred_element_type=F32)
                + around(acc, way).astype(F32)
            ).astype(BF16)
            for (way, weight), acc in zip(lanes, accs)
        ]
    return jnp.concatenate(accs, axis=1)[None]


def solution(mesh):
    rows = P(("shift", "dp"), "sp", None, None)
    return jax.shard_map(
        body,
        mesh=mesh,
        in_specs=(rows, rows, rows, P(("shift", "dp"), None)),
        out_specs=P(("shift", "dp"), "sp", None),
        check_vma=False,
    )
```

```python
import functools
import math

import jax
import jax.numpy as jnp
from jax import lax
from jax.experimental import pallas as pl
from jax.experimental.pallas import tpu as pltpu
from jax.sharding import PartitionSpec as P


F32, BF16 = jnp.float32, jnp.bfloat16
CHUNKS = 2
MIB = 1 << 20


def ring_order(n):
    side = math.isqrt(n)
    if side * side != n or side % 2:
        return list(range(n))
    order = list(range(side))
    for row in range(1, side):
        cols = range(1, side)
        order += [row * side + c for c in (reversed(cols) if row % 2 else cols)]
    order += [row * side for row in range(side - 1, 0, -1)]
    return order


def feature_map(values):
    wide = values.astype(F32)
    return jnp.where(wide > 0.0, wide + 1.0, jnp.exp(jnp.minimum(wide, 0.0))).astype(BF16)


def cost(flops, nbytes):
    return pl.CostEstimate(flops=flops, bytes_accessed=nbytes, transcendentals=0)


def split_mass(mass):
    high = mass.astype(BF16)
    low = (mass - high.astype(F32)).astype(BF16)
    return jnp.concatenate([high, low], axis=0)


def state_kernel(parts, table, here, place, key, value, *refs):
    outs, (keys, values, states) = refs[:parts], refs[parts:]
    tokens, heads, size = key.shape[1:]
    rows = heads * size // parts
    feature = feature_map(key[0]).astype(F32)
    mass = split_mass(jnp.sum(feature, axis=0))
    keys[...] = feature.reshape(tokens * heads, size)
    values[...] = value[0].astype(F32).reshape(tokens * heads, size)
    for h in range(heads):
        states[h * size : (h + 1) * size, :] = lax.dot_general(
            keys[pl.ds(h, tokens, stride=heads), :].astype(BF16),
            values[pl.ds(h, tokens, stride=heads), :].astype(BF16),
            (((0,), (0,)), ((), ())),
            preferred_element_type=F32,
        )
    for j in range(parts):
        start = pl.multiple_of(lax.rem(place[0] + j, parts) * rows, rows)
        outs[j][0, :rows, :] = states[pl.ds(start, rows), :].astype(BF16)
        outs[j][0, rows:, :] = mass


def partial_states(key, value, table, here, place, blocks, heads, parts):
    _, tokens, _, size = key.shape
    rows = heads * size // parts + 2 * heads
    block = pl.BlockSpec((1, tokens, heads, size), lambda i, t, d, p: (0, 0, t[d[0] * blocks + i], 0))
    return pl.pallas_call(
        functools.partial(state_kernel, parts),
        grid_spec=pltpu.PrefetchScalarGridSpec(
            num_scalar_prefetch=3,
            grid=(blocks,),
            in_specs=[block, block],
            out_specs=[pl.BlockSpec((1, rows, size), lambda i, t, d, p: (i, 0, 0))] * parts,
            scratch_shapes=[
                pltpu.VMEM((tokens * heads, size), F32),
                pltpu.VMEM((tokens * heads, size), F32),
                pltpu.VMEM((heads * size, size), F32),
            ],
        ),
        out_shape=[jax.ShapeDtypeStruct((blocks, rows, size), BF16)] * parts,
        cost_estimate=cost(blocks * heads * tokens * size * size * 2, blocks * heads * tokens * size * 4),
        compiler_params=pltpu.CompilerParams(vmem_limit_bytes=56 * MIB),
        name="partial_states",
    )(table, here, place, key, value)


def total_kernel(blocks, heads, count, *refs):
    takes, outs = refs[:-blocks], refs[-blocks:]
    rows = takes[0].shape[1] - 2 * heads
    for b in range(blocks):
        total = takes[0][b].astype(F32)
        for take in takes[1:]:
            total = total + take[b].astype(F32)
        total = total / count
        outs[b][:rows, :] = total[:rows].astype(BF16)
        mass = total[rows : rows + heads] + total[rows + heads :]
        outs[b][rows:, :] = split_mass(mass)


def total_states(takes, heads, count):
    blocks, rows, size = takes[0].shape
    return pl.pallas_call(
        functools.partial(total_kernel, blocks, heads, count),
        out_shape=[jax.ShapeDtypeStruct((rows, size), BF16)] * blocks,
        cost_estimate=cost(blocks * rows * size * 8, blocks * rows * size * 10),
        compiler_params=pltpu.CompilerParams(vmem_limit_bytes=8 * MIB),
        name="total_states",
    )(*takes)


def read_kernel(parts, scale, block, place, query, mass, *refs):
    pieces, (out, queries, states) = refs[:parts], refs[parts:]
    tokens, heads, size = query.shape[1:]
    rows = heads * size // parts
    for j in range(parts):
        start = pl.multiple_of(lax.rem(place[0] + parts - j, parts) * rows, rows)
        states[pl.ds(start, rows), :] = pieces[j][0, :rows, :]
    queries[...] = feature_map(query[0]).astype(F32).reshape(tokens * heads, size)
    masses = mass[...].astype(F32)
    masses = (masses[:heads] + masses[heads:]).T
    none = jnp.zeros((size, size), BF16)
    for h in range(heads):
        feature = queries[pl.ds(h, tokens, stride=heads), :].astype(BF16)
        whole = jnp.broadcast_to(masses[:, h : h + 1], (size, size))
        high = whole.astype(BF16)
        low = (whole - high.astype(F32)).astype(BF16)
        state = jnp.concatenate([states[h * size : (h + 1) * size, :], none], axis=0)
        both = jnp.concatenate([state, jnp.concatenate([high, low], axis=0)], axis=1)
        read = jnp.dot(
            jnp.concatenate([feature, feature], axis=1), both, preferred_element_type=F32
        )
        result = read[:, :size] / (read[:, size:] + 0.001) * scale
        out[:, h * size : (h + 1) * size] = result.astype(BF16)


def read_states(query, own, pieces, slot, block, heads, place, scale):
    parts = len(pieces)
    _, tokens, _, size = query.shape
    rows = own.shape[0]
    return pl.pallas_call(
        functools.partial(read_kernel, parts, scale),
        grid_spec=pltpu.PrefetchScalarGridSpec(
            num_scalar_prefetch=2,
            grid=(1,),
            in_specs=[
                pl.BlockSpec((1, tokens, heads, size), lambda i, b, p: (0, 0, b[0], 0)),
                pl.BlockSpec((2 * heads, size), lambda i, b, p: (rows // (2 * heads) - 1, 0)),
            ]
            + [pl.BlockSpec((1, rows, size), lambda i, b, p: (slot, 0, 0))] * parts,
            out_specs=pl.BlockSpec((tokens, heads * size), lambda i, b, p: (0, 0)),
            scratch_shapes=[
                pltpu.VMEM((tokens * heads, size), F32),
                pltpu.VMEM((heads * size, size), BF16),
            ],
        ),
        out_shape=jax.ShapeDtypeStruct((tokens, heads * size), BF16),
        cost_estimate=cost(heads * tokens * size * size * 8, heads * tokens * size * 4),
        compiler_params=pltpu.CompilerParams(vmem_limit_bytes=12 * MIB),
        name="read_states",
    )(block, place, query, own, *pieces)


def partial_states_plain(key, value, table, here, place, blocks, heads, parts):
    _, _, _, size = key.shape
    outs = [[] for _ in range(parts)]
    for b in range(blocks):
        start = table[here[0] * blocks + b] * heads
        key_block = feature_map(lax.dynamic_slice_in_dim(key[0], start, heads, 1))
        value_block = lax.dynamic_slice_in_dim(value[0], start, heads, 1)
        state = jnp.einsum("thd,the->hde", key_block, value_block, preferred_element_type=F32)
        state = state.reshape(heads * size, size).astype(BF16)
        mass = split_mass(jnp.sum(key_block.astype(F32), axis=0))
        rows = heads * size // parts
        for j in range(parts):
            piece = lax.dynamic_slice_in_dim(state, lax.rem(place[0] + j, parts) * rows, rows, 0)
            outs[j].append(jnp.concatenate([piece, mass]))
    return [jnp.stack(out) for out in outs]


def total_states_plain(takes, heads, count):
    total = sum(take.astype(F32) for take in takes) / count
    rows = total.shape[1] - 2 * heads
    mass = total[:, rows : rows + heads] + total[:, rows + heads :]
    return [
        jnp.concatenate([total[b, :rows].astype(BF16), split_mass(mass[b])])
        for b in range(total.shape[0])
    ]


def read_states_plain(query, own, pieces, slot, block, heads, place, scale):
    parts = len(pieces)
    _, tokens, _, size = query.shape
    query = lax.dynamic_slice_in_dim(query[0], block[0] * heads, heads, 1)
    mass = own[-2 * heads :].astype(F32)
    stack = jnp.stack([piece[slot, : -2 * heads] for piece in pieces])
    order = lax.rem(place[0] + parts - jnp.arange(parts), parts)
    state = stack[order].reshape(heads, size, size)
    feature = feature_map(query)
    top = jnp.einsum("thd,hde->the", feature, state, preferred_element_type=F32)
    bottom = jnp.einsum(
        "thd,hd->th",
        feature.astype(F32),
        mass[:heads] + mass[heads:],
        precision=lax.Precision.HIGHEST,
    )
    read = top / (bottom + 0.001)[..., None] * scale
    return read.astype(BF16).reshape(tokens, heads * size)


def layer(query_rows, key_rows, value_rows, out_weight):
    n, parts = lax.axis_size("dp"), lax.axis_size("sp")
    _, tokens, all_heads, size = query_rows.shape
    heads, width = all_heads // n, out_weight.shape[1]
    count = tokens * parts
    fits = heads % 8 == 0 and (heads * size) % (16 * parts) == 0
    make_partial = partial_states if fits else partial_states_plain
    make_total = total_states if fits else total_states_plain
    make_read = read_states if fits else read_states_plain

    ring = ring_order(n)
    to = [[ring[(ring.index(d) + o) % n] for o in range(n)] for d in range(n)]
    here = lax.axis_index("dp").reshape(1)
    place = lax.axis_index("sp").reshape(1)

    def block_of(offset):
        found = jnp.int32(to[0][offset])
        for d in range(1, n):
            found = jnp.where(here[0] == d, to[d][offset], found)
        return found

    def around(x, offset):
        return lax.ppermute(x, "dp", [(d, to[d][offset % n]) for d in range(n)])

    def along(x, offset):
        return lax.ppermute(x, "sp", [(i, (i + offset) % parts) for i in range(parts)])

    groups = [sorted({1, n - 1}), list(range(2, n - 1)) + [0]] if n > 1 else [[0]]

    takes, queries, mixed = [], {}, {}
    for group in groups:
        table = jnp.array([to[d][o] for d in range(n) for o in group], jnp.int32)
        sent = make_partial(key_rows, value_rows, table, here, place, len(group), heads, parts)
        takes.append([sent[0]] + [along(sent[j], j) for j in range(1, parts)])
        for o in group:
            if o:
                piece = lax.dynamic_slice_in_dim(query_rows, block_of(o) * heads, heads, 2)
                queries[-o % n] = around(piece, o)
    for group, take in zip(groups, takes):
        totals = make_total(take, heads, count)
        owns = [around(totals[i], o) if o else totals[i] for i, o in enumerate(group)]
        stack = jnp.stack(owns)
        pieces = [stack] + [along(stack, j) for j in range(1, parts)]
        for i, o in enumerate(group):
            slot = -o % n
            query, block = (queries[slot], jnp.zeros(1, jnp.int32)) if o else (query_rows, here)
            mixed[slot] = make_read(
                query, owns[i], pieces, i, block, heads, place, count**0.5
            )

    lanes = []
    step = width // (2 * CHUNKS)
    for c in range(2 * CHUNKS):
        way = 1 if c % 2 == 0 else -1
        lanes.append((way, out_weight[:, c * step : (c + 1) * step]))
    accs = []
    for way, weight in lanes:
        acc = jnp.dot(mixed[-way % n], weight, preferred_element_type=F32).astype(BF16)
        accs.append(acc)
    for k in range(1, n):
        for lane, (way, weight) in enumerate(lanes):
            taken = around(accs[lane], way).astype(F32)
            product = jnp.dot(mixed[-way * (k + 1) % n], weight, preferred_element_type=F32)
            accs[lane] = (product + taken).astype(BF16)
    return jnp.concatenate(accs, axis=1)[None]


def solution(mesh):
    rows = P(("shift", "dp"), "sp", None, None)
    return jax.shard_map(
        layer,
        mesh=mesh,
        in_specs=(rows, rows, rows, P(("shift", "dp"), None)),
        out_specs=P(("shift", "dp"), "sp", None),
        check_vma=False,
    )
```

```python
import functools
import math

import jax
import jax.numpy as jnp
from jax import lax
from jax.experimental import pallas as pl
from jax.experimental.pallas import tpu as pltpu
from jax.sharding import PartitionSpec as P


F32, BF16 = jnp.float32, jnp.bfloat16
CHUNKS = 2
MIB = 1 << 20


def ring_order(n):
    side = math.isqrt(n)
    if side * side != n or side % 2:
        return list(range(n))
    order = list(range(side))
    for row in range(1, side):
        cols = range(1, side)
        order += [row * side + c for c in (reversed(cols) if row % 2 else cols)]
    order += [row * side for row in range(side - 1, 0, -1)]
    return order


def feature_map(values):
    wide = values.astype(F32)
    return jnp.where(wide > 0.0, wide + 1.0, jnp.exp(jnp.minimum(wide, 0.0))).astype(BF16)


def weight_bytes(weight):
    return weight.size * weight.dtype.itemsize


def cost(flops, nbytes):
    return pl.CostEstimate(flops=flops, bytes_accessed=nbytes, transcendentals=0)


def split_mass(mass):
    high = mass.astype(BF16)
    low = (mass - high.astype(F32)).astype(BF16)
    return jnp.concatenate([high, low], axis=0)


def state_kernel(parts, table, here, place, key, value, *refs):
    outs, (keys, values, states) = refs[:-3], refs[-3:]
    tokens, heads, size = key.shape[1:]
    rows = heads * size // parts
    feature = feature_map(key[0]).astype(F32)
    mass = split_mass(jnp.sum(feature, axis=0))
    keys[...] = feature.reshape(tokens * heads, size)
    values[...] = value[0].astype(F32).reshape(tokens * heads, size)
    for h in range(heads):
        states[h * size : (h + 1) * size, :] = lax.dot_general(
            keys[pl.ds(h, tokens, stride=heads), :].astype(BF16),
            values[pl.ds(h, tokens, stride=heads), :].astype(BF16),
            (((0,), (0,)), ((), ())),
            preferred_element_type=F32,
        )
    for j in range(parts):
        start = pl.multiple_of(lax.rem(place[0] + j, parts) * rows, rows)
        out = outs[j].at[0] if len(outs) == parts else outs[0].at[0, j]
        out[:rows, :] = states[pl.ds(start, rows), :].astype(BF16)
        out[rows:, :] = mass


def partial_states(key, value, table, here, place, blocks, heads, parts, grant, joined):
    _, tokens, _, size = key.shape
    rows = heads * size // parts + 2 * heads
    if joined:
        outs = [jax.ShapeDtypeStruct((blocks, parts, rows, size), BF16)]
        out_specs = [pl.BlockSpec((1, parts, rows, size), lambda i, t, d, p: (i, 0, 0, 0))]
    else:
        outs = [jax.ShapeDtypeStruct((blocks, rows, size), BF16)] * parts
        out_specs = [pl.BlockSpec((1, rows, size), lambda i, t, d, p: (i, 0, 0))] * parts
    block = pl.BlockSpec((1, tokens, heads, size), lambda i, t, d, p: (0, 0, t[d[0] * blocks + i], 0))
    return pl.pallas_call(
        functools.partial(state_kernel, parts),
        grid_spec=pltpu.PrefetchScalarGridSpec(
            num_scalar_prefetch=3,
            grid=(blocks,),
            in_specs=[block, block],
            out_specs=out_specs,
            scratch_shapes=[
                pltpu.VMEM((tokens * heads, size), F32),
                pltpu.VMEM((tokens * heads, size), F32),
                pltpu.VMEM((heads * size, size), F32),
            ],
        ),
        out_shape=outs,
        cost_estimate=cost(blocks * heads * tokens * size * size * 2, blocks * heads * tokens * size * 4),
        compiler_params=pltpu.CompilerParams(vmem_limit_bytes=grant * MIB),
        name="partial_states",
    )(table, here, place, key, value)


def total_kernel(blocks, heads, count, *refs):
    takes, outs = refs[:-blocks], refs[-blocks:]
    rows = takes[0].shape[1] - 2 * heads
    for b in range(blocks):
        total = takes[0][b].astype(F32)
        for take in takes[1:]:
            total = total + take[b].astype(F32)
        total = total / count
        outs[b][:rows, :] = total[:rows].astype(BF16)
        mass = total[rows : rows + heads] + total[rows + heads :]
        outs[b][rows:, :] = split_mass(mass)


def total_states(takes, heads, count):
    blocks, rows, size = takes[0].shape
    return pl.pallas_call(
        functools.partial(total_kernel, blocks, heads, count),
        out_shape=[jax.ShapeDtypeStruct((rows, size), BF16)] * blocks,
        cost_estimate=cost(blocks * rows * size * 8, blocks * rows * size * 10),
        compiler_params=pltpu.CompilerParams(vmem_limit_bytes=8 * MIB),
        name="total_states",
    )(*takes)


def read_kernel(parts, scale, block, place, query, mass, *refs):
    pieces, (out, queries, states) = refs[:parts], refs[parts:]
    tokens, heads, size = query.shape[1:]
    rows = heads * size // parts
    for j in range(parts):
        start = pl.multiple_of(lax.rem(place[0] + parts - j, parts) * rows, rows)
        states[pl.ds(start, rows), :] = pieces[j][0, :rows, :]
    queries[...] = feature_map(query[0]).astype(F32).reshape(tokens * heads, size)
    masses = mass[...].astype(F32)
    masses = (masses[:heads] + masses[heads:]).T
    none = jnp.zeros((size, size), BF16)
    for h in range(heads):
        feature = queries[pl.ds(h, tokens, stride=heads), :].astype(BF16)
        whole = jnp.broadcast_to(masses[:, h : h + 1], (size, size))
        high = whole.astype(BF16)
        low = (whole - high.astype(F32)).astype(BF16)
        state = jnp.concatenate([states[h * size : (h + 1) * size, :], none], axis=0)
        both = jnp.concatenate([state, jnp.concatenate([high, low], axis=0)], axis=1)
        read = jnp.dot(
            jnp.concatenate([feature, feature], axis=1), both, preferred_element_type=F32
        )
        result = read[:, :size] / (read[:, size:] + 0.001) * scale
        out[:, h * size : (h + 1) * size] = result.astype(BF16)


def read_states(query, own, pieces, slot, block, heads, place, scale):
    parts = len(pieces)
    _, tokens, _, size = query.shape
    rows = own.shape[0]
    return pl.pallas_call(
        functools.partial(read_kernel, parts, scale),
        grid_spec=pltpu.PrefetchScalarGridSpec(
            num_scalar_prefetch=2,
            grid=(1,),
            in_specs=[
                pl.BlockSpec((1, tokens, heads, size), lambda i, b, p: (0, 0, b[0], 0)),
                pl.BlockSpec((2 * heads, size), lambda i, b, p: (rows // (2 * heads) - 1, 0)),
            ]
            + [pl.BlockSpec((1, rows, size), lambda i, b, p: (slot, 0, 0))] * parts,
            out_specs=pl.BlockSpec((tokens, heads * size), lambda i, b, p: (0, 0)),
            scratch_shapes=[
                pltpu.VMEM((tokens * heads, size), F32),
                pltpu.VMEM((heads * size, size), BF16),
            ],
        ),
        out_shape=jax.ShapeDtypeStruct((tokens, heads * size), BF16),
        cost_estimate=cost(heads * tokens * size * size * 8, heads * tokens * size * 4),
        compiler_params=pltpu.CompilerParams(vmem_limit_bytes=12 * MIB),
        name="read_states",
    )(block, place, query, own, *pieces)


def hold_kernel(weight, out, sem):
    copy = pltpu.make_async_copy(weight, out, sem)
    copy.start()
    copy.wait()


def hold(weight):
    return pl.pallas_call(
        hold_kernel,
        in_specs=[pl.BlockSpec(memory_space=pl.ANY)],
        out_specs=pl.BlockSpec(memory_space=pltpu.VMEM),
        scratch_shapes=[pltpu.SemaphoreType.DMA],
        out_shape=jax.ShapeDtypeStruct(weight.shape, weight.dtype),
        compiler_params=pltpu.CompilerParams(vmem_limit_bytes=weight_bytes(weight) + MIB),
        name="hold",
    )(weight)


def partial_states_plain(key, value, table, here, place, blocks, heads, parts, grant, joined):
    _, _, _, size = key.shape
    outs = [[] for _ in range(parts)]
    for b in range(blocks):
        start = table[here[0] * blocks + b] * heads
        key_block = feature_map(lax.dynamic_slice_in_dim(key[0], start, heads, 1))
        value_block = lax.dynamic_slice_in_dim(value[0], start, heads, 1)
        state = jnp.einsum("thd,the->hde", key_block, value_block, preferred_element_type=F32)
        state = state.reshape(heads * size, size).astype(BF16)
        mass = split_mass(jnp.sum(key_block.astype(F32), axis=0))
        rows = heads * size // parts
        for j in range(parts):
            piece = lax.dynamic_slice_in_dim(state, lax.rem(place[0] + j, parts) * rows, rows, 0)
            outs[j].append(jnp.concatenate([piece, mass]))
    outs = [jnp.stack(out) for out in outs]
    return [jnp.stack(outs, axis=1)] if joined else outs


def total_states_plain(takes, heads, count):
    total = sum(take.astype(F32) for take in takes) / count
    rows = total.shape[1] - 2 * heads
    mass = total[:, rows : rows + heads] + total[:, rows + heads :]
    return [
        jnp.concatenate([total[b, :rows].astype(BF16), split_mass(mass[b])])
        for b in range(total.shape[0])
    ]


def read_states_plain(query, own, pieces, slot, block, heads, place, scale):
    parts = len(pieces)
    _, tokens, _, size = query.shape
    query = lax.dynamic_slice_in_dim(query[0], block[0] * heads, heads, 1)
    mass = own[-2 * heads :].astype(F32)
    stack = jnp.stack([piece[slot, : -2 * heads] for piece in pieces])
    order = lax.rem(place[0] + parts - jnp.arange(parts), parts)
    state = stack[order].reshape(heads, size, size)
    feature = feature_map(query)
    top = jnp.einsum("thd,hde->the", feature, state, preferred_element_type=F32)
    bottom = jnp.einsum(
        "thd,hd->th",
        feature.astype(F32),
        mass[:heads] + mass[heads:],
        precision=lax.Precision.HIGHEST,
    )
    read = top / (bottom + 0.001)[..., None] * scale
    return read.astype(BF16).reshape(tokens, heads * size)


def layer(query_rows, key_rows, value_rows, out_weight):
    n, parts = lax.axis_size("dp"), lax.axis_size("sp")
    _, tokens, all_heads, size = query_rows.shape
    heads, width = all_heads // n, out_weight.shape[1]
    count = tokens * parts
    fits = heads % 8 == 0 and (heads * size) % (16 * parts) == 0
    make_partial = partial_states if fits else partial_states_plain
    make_total = total_states if fits else total_states_plain
    make_read = read_states if fits else read_states_plain

    ring = ring_order(n)
    to = [[ring[(ring.index(d) + o) % n] for o in range(n)] for d in range(n)]
    here = lax.axis_index("dp").reshape(1)
    place = lax.axis_index("sp").reshape(1)

    def block_of(offset):
        found = jnp.int32(to[0][offset])
        for d in range(1, n):
            found = jnp.where(here[0] == d, to[d][offset], found)
        return found

    def around(x, offset):
        return lax.ppermute(x, "dp", [(d, to[d][offset % n]) for d in range(n)])

    def along(x, offset):
        return lax.ppermute(x, "sp", [(i, (i + offset) % parts) for i in range(parts)])

    groups = [g for g in (sorted({1, n - 1} - {n, 0}), list(range(2, n - 1)), [0]) if g]

    takes, queries, mixed = [], {}, {}
    step = width // (2 * CHUNKS)
    for g, group in enumerate(groups):
        table = jnp.array([to[d][o] for d in range(n) for o in group], jnp.int32)
        size_of = (len(group), heads, parts, 16 if g else 56)
        far = g > 0 and group[0] > 0
        sent = make_partial(key_rows, value_rows, table, here, place, *size_of, far)
        if far:
            moved = [around(sent[0][i], o) for i, o in enumerate(group)]
            sent = [jnp.stack([x[j] for x in moved]) for j in range(parts)]
        takes.append([sent[0]] + [along(sent[j], j) for j in range(1, parts)])
        for o in group:
            if o:
                piece = lax.dynamic_slice_in_dim(query_rows, block_of(o) * heads, heads, 2)
                queries[-o % n] = around(piece, o)
    for g, (group, take) in enumerate(zip(groups, takes)):
        owns = list(make_total(take, heads, count))
        if g == 0:
            owns = [around(own, o) if o else own for own, o in zip(owns, group)]
        stack = jnp.stack(owns) if len(owns) > 1 else owns[0][None]
        pieces = [stack] + [along(stack, j) for j in range(1, parts)]
        for i, o in enumerate(group):
            slot = -o % n
            query, block = (queries[slot], jnp.zeros(1, jnp.int32)) if o else (query_rows, here)
            mixed[slot] = make_read(
                query, owns[i], pieces, i, block, heads, place, count**0.5
            )

    if fits and weight_bytes(out_weight) <= 16 * MIB:
        out_weight = hold(out_weight)

    lanes = []
    for c in range(2 * CHUNKS):
        way = 1 if c % 2 == 0 else -1
        lanes.append((way, out_weight[:, c * step : (c + 1) * step]))
    accs = []
    for way, weight in lanes:
        acc = jnp.dot(mixed[-way % n], weight, preferred_element_type=F32).astype(BF16)
        accs.append(acc)
    for k in range(1, n):
        for lane, (way, weight) in enumerate(lanes):
            accs[lane] = around(accs[lane], way).astype(F32)
            if k < n - 1:
                product = jnp.dot(mixed[-way * (k + 1) % n], weight, preferred_element_type=F32)
                accs[lane] = (product + accs[lane]).astype(BF16)
    product = jnp.dot(mixed[0], out_weight, preferred_element_type=F32)
    product = lax.optimization_barrier(product)
    return (product + jnp.concatenate(accs, axis=1)).astype(BF16)[None]


def solution(mesh):
    rows = P(("shift", "dp"), "sp", None, None)
    return jax.shard_map(
        layer,
        mesh=mesh,
        in_specs=(rows, rows, rows, P(("shift", "dp"), None)),
        out_specs=P(("shift", "dp"), "sp", None),
        check_vma=False,
    )
```

```python
import functools
import math

import jax
import jax.numpy as jnp
from jax import lax
from jax.experimental import pallas as pl
from jax.experimental.pallas import tpu as pltpu
from jax.sharding import PartitionSpec as P


F32, BF16 = jnp.float32, jnp.bfloat16
CHUNKS = 2
MIB = 1 << 20


def ring_order(n):
    side = math.isqrt(n)
    if side * side != n or side % 2:
        return list(range(n))
    order = list(range(side))
    for row in range(1, side):
        cols = range(1, side)
        order += [row * side + c for c in (reversed(cols) if row % 2 else cols)]
    order += [row * side for row in range(side - 1, 0, -1)]
    return order


def feature_map(values):
    wide = values.astype(F32)
    return jnp.where(wide > 0.0, wide + 1.0, jnp.exp(jnp.minimum(wide, 0.0))).astype(BF16)


def weight_bytes(weight):
    return weight.size * weight.dtype.itemsize


def cost(flops, nbytes):
    return pl.CostEstimate(flops=flops, bytes_accessed=nbytes, transcendentals=0)


def split_mass(mass):
    high = mass.astype(BF16)
    low = (mass - high.astype(F32)).astype(BF16)
    return jnp.concatenate([high, low], axis=0)


def state_kernel(parts, table, here, place, key, value, *refs):
    outs, (keys, values, states) = refs[:-3], refs[-3:]
    tokens, heads, size = key.shape[1:]
    rows = heads * size // parts
    feature = feature_map(key[0]).astype(F32)
    mass = split_mass(jnp.sum(feature, axis=0))
    keys[...] = feature.reshape(tokens * heads, size)
    values[...] = value[0].astype(F32).reshape(tokens * heads, size)
    for h in range(heads):
        states[h * size : (h + 1) * size, :] = lax.dot_general(
            keys[pl.ds(h, tokens, stride=heads), :].astype(BF16),
            values[pl.ds(h, tokens, stride=heads), :].astype(BF16),
            (((0,), (0,)), ((), ())),
            preferred_element_type=F32,
        )
    for j in range(parts):
        start = pl.multiple_of(lax.rem(place[0] + j, parts) * rows, rows)
        out = outs[j].at[0] if len(outs) == parts else outs[0].at[0, j]
        out[:rows, :] = states[pl.ds(start, rows), :].astype(BF16)
        out[rows:, :] = mass


def partial_states(key, value, table, here, place, blocks, heads, parts, grant, joined):
    _, tokens, _, size = key.shape
    rows = heads * size // parts + 2 * heads
    if joined:
        outs = [jax.ShapeDtypeStruct((blocks, parts, rows, size), BF16)]
        out_specs = [pl.BlockSpec((1, parts, rows, size), lambda i, t, d, p: (i, 0, 0, 0))]
    else:
        outs = [jax.ShapeDtypeStruct((blocks, rows, size), BF16)] * parts
        out_specs = [pl.BlockSpec((1, rows, size), lambda i, t, d, p: (i, 0, 0))] * parts
    block = pl.BlockSpec((1, tokens, heads, size), lambda i, t, d, p: (0, 0, t[d[0] * blocks + i], 0))
    return pl.pallas_call(
        functools.partial(state_kernel, parts),
        grid_spec=pltpu.PrefetchScalarGridSpec(
            num_scalar_prefetch=3,
            grid=(blocks,),
            in_specs=[block, block],
            out_specs=out_specs,
            scratch_shapes=[
                pltpu.VMEM((tokens * heads, size), F32),
                pltpu.VMEM((tokens * heads, size), F32),
                pltpu.VMEM((heads * size, size), F32),
            ],
        ),
        out_shape=outs,
        cost_estimate=cost(blocks * heads * tokens * size * size * 2, blocks * heads * tokens * size * 4),
        compiler_params=pltpu.CompilerParams(vmem_limit_bytes=grant * MIB),
        name="partial_states",
    )(table, here, place, key, value)


def total_kernel(blocks, heads, count, *refs):
    takes, outs = refs[:-blocks], refs[-blocks:]
    rows = takes[0].shape[1] - 2 * heads
    for b in range(blocks):
        total = takes[0][b].astype(F32)
        for take in takes[1:]:
            total = total + take[b].astype(F32)
        total = total / count
        outs[b][:rows, :] = total[:rows].astype(BF16)
        mass = total[rows : rows + heads] + total[rows + heads :]
        outs[b][rows:, :] = split_mass(mass)


def total_states(takes, heads, count):
    blocks, rows, size = takes[0].shape
    return pl.pallas_call(
        functools.partial(total_kernel, blocks, heads, count),
        out_shape=[jax.ShapeDtypeStruct((rows, size), BF16)] * blocks,
        cost_estimate=cost(blocks * rows * size * 8, blocks * rows * size * 10),
        compiler_params=pltpu.CompilerParams(vmem_limit_bytes=8 * MIB),
        name="total_states",
    )(*takes)


def read_kernel(parts, scale, block, place, mass, *refs):
    pieces, asked, (out, queries, states) = refs[:parts], refs[parts:-3], refs[-3:]
    heads, size = asked[0].shape[2:]
    tokens = out.shape[0]
    rows = heads * size // parts
    for j in range(parts):
        start = pl.multiple_of(lax.rem(place[0] + parts - j, parts) * rows, rows)
        states[pl.ds(start, rows), :] = pieces[j][0, :rows, :]
    done = 0
    for query in asked:
        some = query.shape[1] * heads
        queries[done : done + some, :] = feature_map(query[0]).astype(F32).reshape(some, size)
        done += some
    masses = mass[...].astype(F32)
    masses = (masses[:heads] + masses[heads:]).T
    none = jnp.zeros((size, size), BF16)
    for h in range(heads):
        feature = queries[pl.ds(h, tokens, stride=heads), :].astype(BF16)
        whole = jnp.broadcast_to(masses[:, h : h + 1], (size, size))
        high = whole.astype(BF16)
        low = (whole - high.astype(F32)).astype(BF16)
        state = jnp.concatenate([states[h * size : (h + 1) * size, :], none], axis=0)
        both = jnp.concatenate([state, jnp.concatenate([high, low], axis=0)], axis=1)
        read = jnp.dot(
            jnp.concatenate([feature, feature], axis=1), both, preferred_element_type=F32
        )
        result = read[:, :size] / (read[:, size:] + 0.001) * scale
        out[:, h * size : (h + 1) * size] = result.astype(BF16)


def read_states(queries, own, pieces, slot, block, heads, place, scale):
    parts = len(pieces)
    tokens, size = sum(query.shape[1] for query in queries), own.shape[1]
    rows = own.shape[0]
    return pl.pallas_call(
        functools.partial(read_kernel, parts, scale),
        grid_spec=pltpu.PrefetchScalarGridSpec(
            num_scalar_prefetch=2,
            grid=(1,),
            in_specs=[pl.BlockSpec((2 * heads, size), lambda i, b, p: (rows // (2 * heads) - 1, 0))]
            + [pl.BlockSpec((1, rows, size), lambda i, b, p: (slot, 0, 0))] * parts
            + [
                pl.BlockSpec((1, query.shape[1], heads, size), lambda i, b, p: (0, 0, b[0], 0))
                for query in queries
            ],
            out_specs=pl.BlockSpec((tokens, heads * size), lambda i, b, p: (0, 0)),
            scratch_shapes=[
                pltpu.VMEM((tokens * heads, size), F32),
                pltpu.VMEM((heads * size, size), BF16),
            ],
        ),
        out_shape=jax.ShapeDtypeStruct((tokens, heads * size), BF16),
        cost_estimate=cost(heads * tokens * size * size * 8, heads * tokens * size * 4),
        compiler_params=pltpu.CompilerParams(vmem_limit_bytes=12 * MIB),
        name="read_states",
    )(block, place, own, *pieces, *queries)


def hold_kernel(weight, out, sem):
    copy = pltpu.make_async_copy(weight, out, sem)
    copy.start()
    copy.wait()


def hold(weight):
    return pl.pallas_call(
        hold_kernel,
        in_specs=[pl.BlockSpec(memory_space=pl.ANY)],
        out_specs=pl.BlockSpec(memory_space=pltpu.VMEM),
        scratch_shapes=[pltpu.SemaphoreType.DMA],
        out_shape=jax.ShapeDtypeStruct(weight.shape, weight.dtype),
        compiler_params=pltpu.CompilerParams(vmem_limit_bytes=weight_bytes(weight) + MIB),
        name="hold",
    )(weight)


def partial_states_plain(key, value, table, here, place, blocks, heads, parts, grant, joined):
    _, _, _, size = key.shape
    outs = [[] for _ in range(parts)]
    for b in range(blocks):
        start = table[here[0] * blocks + b] * heads
        key_block = feature_map(lax.dynamic_slice_in_dim(key[0], start, heads, 1))
        value_block = lax.dynamic_slice_in_dim(value[0], start, heads, 1)
        state = jnp.einsum("thd,the->hde", key_block, value_block, preferred_element_type=F32)
        state = state.reshape(heads * size, size).astype(BF16)
        mass = split_mass(jnp.sum(key_block.astype(F32), axis=0))
        rows = heads * size // parts
        for j in range(parts):
            piece = lax.dynamic_slice_in_dim(state, lax.rem(place[0] + j, parts) * rows, rows, 0)
            outs[j].append(jnp.concatenate([piece, mass]))
    outs = [jnp.stack(out) for out in outs]
    return [jnp.stack(outs, axis=1)] if joined else outs


def total_states_plain(takes, heads, count):
    total = sum(take.astype(F32) for take in takes) / count
    rows = total.shape[1] - 2 * heads
    mass = total[:, rows : rows + heads] + total[:, rows + heads :]
    return [
        jnp.concatenate([total[b, :rows].astype(BF16), split_mass(mass[b])])
        for b in range(total.shape[0])
    ]


def read_states_plain(queries, own, pieces, slot, block, heads, place, scale):
    parts = len(pieces)
    query = jnp.concatenate(queries, axis=1)[0]
    tokens, _, size = query.shape
    query = lax.dynamic_slice_in_dim(query, block[0] * heads, heads, 1)
    mass = own[-2 * heads :].astype(F32)
    stack = jnp.stack([piece[slot, : -2 * heads] for piece in pieces])
    order = lax.rem(place[0] + parts - jnp.arange(parts), parts)
    state = stack[order].reshape(heads, size, size)
    feature = feature_map(query)
    top = jnp.einsum("thd,hde->the", feature, state, preferred_element_type=F32)
    bottom = jnp.einsum(
        "thd,hd->th",
        feature.astype(F32),
        mass[:heads] + mass[heads:],
        precision=lax.Precision.HIGHEST,
    )
    read = top / (bottom + 0.001)[..., None] * scale
    return read.astype(BF16).reshape(tokens, heads * size)


def layer(query_rows, key_rows, value_rows, out_weight):
    n, parts = lax.axis_size("dp"), lax.axis_size("sp")
    _, tokens, all_heads, size = query_rows.shape
    heads, width = all_heads // n, out_weight.shape[1]
    count = tokens * parts
    fits = heads % 8 == 0 and (heads * size) % (16 * parts) == 0
    make_partial = partial_states if fits else partial_states_plain
    make_total = total_states if fits else total_states_plain
    make_read = read_states if fits else read_states_plain

    ring = ring_order(n)
    to = [[ring[(ring.index(d) + o) % n] for o in range(n)] for d in range(n)]
    here = lax.axis_index("dp").reshape(1)
    place = lax.axis_index("sp").reshape(1)

    def block_of(offset):
        found = jnp.int32(to[0][offset])
        for d in range(1, n):
            found = jnp.where(here[0] == d, to[d][offset], found)
        return found

    def around(x, offset):
        return lax.ppermute(x, "dp", [(d, to[d][offset % n]) for d in range(n)])

    def along(x, offset):
        return lax.ppermute(x, "sp", [(i, (i + offset) % parts) for i in range(parts)])

    groups = [g for g in (sorted({1, n - 1} - {n, 0}), list(range(2, n - 1)), [0]) if g]

    takes, queries, mixed = [], {}, {}
    step = width // (2 * CHUNKS)
    for g, group in enumerate(groups):
        table = jnp.array([to[d][o] for d in range(n) for o in group], jnp.int32)
        size_of = (len(group), heads, parts, 16 if g else 56)
        far = g > 0 and group[0] > 0
        sent = make_partial(key_rows, value_rows, table, here, place, *size_of, far)
        if far:
            moved = [around(sent[0][i], o) for i, o in enumerate(group)]
            sent = [jnp.stack([x[j] for x in moved]) for j in range(parts)]
        takes.append([sent[0]] + [along(sent[j], j) for j in range(1, parts)])
        halves = [tokens // 4] if far else 1
        for o in group:
            if o:
                piece = lax.dynamic_slice_in_dim(query_rows, block_of(o) * heads, heads, 2)
                cuts = jnp.split(piece, halves, axis=1)
                for c, cut in enumerate(cuts):
                    cuts[c] = around(cut, o)
                queries[-o % n] = cuts
    for g, (group, take) in enumerate(zip(groups, takes)):
        owns = list(make_total(take, heads, count))
        if g == 0:
            owns = [around(own, o) if o else own for own, o in zip(owns, group)]
        stack = jnp.stack(owns) if len(owns) > 1 else owns[0][None]
        pieces = [stack] + [along(stack, j) for j in range(1, parts)]
        for i, o in enumerate(group):
            slot = -o % n
            query, block = (queries[slot], jnp.zeros(1, jnp.int32)) if o else ([query_rows], here)
            mixed[slot] = make_read(
                query, owns[i], pieces, i, block, heads, place, count**0.5
            )

    if fits and weight_bytes(out_weight) <= 16 * MIB:
        out_weight = hold(out_weight)

    lanes = []
    for c in range(2 * CHUNKS):
        way = 1 if c % 2 == 0 else -1
        lanes.append((way, out_weight[:, c * step : (c + 1) * step]))
    accs = []
    for way, weight in lanes:
        acc = jnp.dot(mixed[-way % n], weight, preferred_element_type=F32).astype(BF16)
        accs.append(acc)
    for k in range(1, n):
        for lane, (way, weight) in enumerate(lanes):
            accs[lane] = around(accs[lane], way).astype(F32)
            if k < n - 1:
                product = jnp.dot(mixed[-way * (k + 1) % n], weight, preferred_element_type=F32)
                accs[lane] = (product + accs[lane]).astype(BF16)
    product = jnp.dot(mixed[0], out_weight, preferred_element_type=F32)
    product = lax.optimization_barrier(product)
    return (product + jnp.concatenate(accs, axis=1)).astype(BF16)[None]


def solution(mesh):
    rows = P(("shift", "dp"), "sp", None, None)
    return jax.shard_map(
        layer,
        mesh=mesh,
        in_specs=(rows, rows, rows, P(("shift", "dp"), None)),
        out_specs=P(("shift", "dp"), "sp", None),
        check_vma=False,
    )
```

```python
import functools
import math

import jax
import jax.numpy as jnp
from jax import lax
from jax.experimental import pallas as pl
from jax.experimental.pallas import tpu as pltpu
from jax.sharding import PartitionSpec as P


F32, BF16 = jnp.float32, jnp.bfloat16
SHARES = (1, 1)
MIB = 1 << 20


def ring_order(n):
    side = math.isqrt(n)
    if side * side != n or side % 2:
        return list(range(n))
    order = list(range(side))
    for row in range(1, side):
        cols = range(1, side)
        order += [row * side + c for c in (reversed(cols) if row % 2 else cols)]
    order += [row * side for row in range(side - 1, 0, -1)]
    return order


def feature_map(values):
    wide = values.astype(F32)
    return jnp.where(wide > 0.0, wide + 1.0, jnp.exp(jnp.minimum(wide, 0.0))).astype(BF16)


def weight_bytes(weight):
    return weight.size * weight.dtype.itemsize


def cost(flops, nbytes):
    return pl.CostEstimate(flops=flops, bytes_accessed=nbytes, transcendentals=0)


def split_mass(mass):
    high = mass.astype(BF16)
    low = (mass - high.astype(F32)).astype(BF16)
    return jnp.concatenate([high, low], axis=0)


def state_kernel(parts, table, here, place, key, value, *refs):
    outs, (keys, values, states) = refs[:-3], refs[-3:]
    tokens, heads, size = key.shape[1:]
    rows = heads * size // parts
    feature = feature_map(key[0]).astype(F32)
    mass = split_mass(jnp.sum(feature, axis=0))
    keys[...] = feature.reshape(tokens * heads, size)
    values[...] = value[0].astype(F32).reshape(tokens * heads, size)
    for h in range(heads):
        states[h * size : (h + 1) * size, :] = lax.dot_general(
            keys[pl.ds(h, tokens, stride=heads), :].astype(BF16),
            values[pl.ds(h, tokens, stride=heads), :].astype(BF16),
            (((0,), (0,)), ((), ())),
            preferred_element_type=F32,
        )
    for j in range(parts):
        start = pl.multiple_of(lax.rem(place[0] + j, parts) * rows, rows)
        out = outs[j].at[0] if len(outs) == parts else outs[0].at[0, j]
        out[:rows, :] = states[pl.ds(start, rows), :].astype(BF16)
        out[rows:, :] = mass


def partial_states(key, value, table, here, place, blocks, heads, parts, grant, joined):
    _, tokens, _, size = key.shape
    rows = heads * size // parts + 2 * heads
    if joined:
        outs = [jax.ShapeDtypeStruct((blocks, parts, rows, size), BF16)]
        out_specs = [pl.BlockSpec((1, parts, rows, size), lambda i, t, d, p: (i, 0, 0, 0))]
    else:
        outs = [jax.ShapeDtypeStruct((blocks, rows, size), BF16)] * parts
        out_specs = [pl.BlockSpec((1, rows, size), lambda i, t, d, p: (i, 0, 0))] * parts
    block = pl.BlockSpec((1, tokens, heads, size), lambda i, t, d, p: (0, 0, t[d[0] * blocks + i], 0))
    return pl.pallas_call(
        functools.partial(state_kernel, parts),
        grid_spec=pltpu.PrefetchScalarGridSpec(
            num_scalar_prefetch=3,
            grid=(blocks,),
            in_specs=[block, block],
            out_specs=out_specs,
            scratch_shapes=[
                pltpu.VMEM((tokens * heads, size), F32),
                pltpu.VMEM((tokens * heads, size), F32),
                pltpu.VMEM((heads * size, size), F32),
            ],
        ),
        out_shape=outs,
        cost_estimate=cost(blocks * heads * tokens * size * size * 2, blocks * heads * tokens * size * 4),
        compiler_params=pltpu.CompilerParams(vmem_limit_bytes=grant * MIB),
        name="partial_states",
    )(table, here, place, key, value)


def total_kernel(blocks, heads, count, *refs):
    takes, outs = refs[:-blocks], refs[-blocks:]
    rows = takes[0].shape[1] - 2 * heads
    for b in range(blocks):
        total = takes[0][b].astype(F32)
        for take in takes[1:]:
            total = total + take[b].astype(F32)
        total = total / count
        outs[b][:rows, :] = total[:rows].astype(BF16)
        mass = total[rows : rows + heads] + total[rows + heads :]
        outs[b][rows:, :] = split_mass(mass)


def total_states(takes, heads, count):
    blocks, rows, size = takes[0].shape
    return pl.pallas_call(
        functools.partial(total_kernel, blocks, heads, count),
        out_shape=[jax.ShapeDtypeStruct((rows, size), BF16)] * blocks,
        cost_estimate=cost(blocks * rows * size * 8, blocks * rows * size * 10),
        compiler_params=pltpu.CompilerParams(vmem_limit_bytes=8 * MIB),
        name="total_states",
    )(*takes)


def read_kernel(parts, scale, block, place, mass, *refs):
    pieces, asked, (out, queries, states) = refs[:parts], refs[parts:-3], refs[-3:]
    heads, size = asked[0].shape[2:]
    tokens = out.shape[0]
    rows = heads * size // parts
    for j in range(parts):
        start = pl.multiple_of(lax.rem(place[0] + parts - j, parts) * rows, rows)
        states[pl.ds(start, rows), :] = pieces[j][0, :rows, :]
    done = 0
    for query in asked:
        some = query.shape[1] * heads
        queries[done : done + some, :] = feature_map(query[0]).astype(F32).reshape(some, size)
        done += some
    masses = mass[...].astype(F32)
    masses = (masses[:heads] + masses[heads:]).T
    none = jnp.zeros((size, size), BF16)
    for h in range(heads):
        feature = queries[pl.ds(h, tokens, stride=heads), :].astype(BF16)
        whole = jnp.broadcast_to(masses[:, h : h + 1], (size, size))
        high = whole.astype(BF16)
        low = (whole - high.astype(F32)).astype(BF16)
        state = jnp.concatenate([states[h * size : (h + 1) * size, :], none], axis=0)
        both = jnp.concatenate([state, jnp.concatenate([high, low], axis=0)], axis=1)
        read = jnp.dot(
            jnp.concatenate([feature, feature], axis=1), both, preferred_element_type=F32
        )
        result = read[:, :size] / (read[:, size:] + 0.001) * scale
        out[:, h * size : (h + 1) * size] = result.astype(BF16)


def read_states(queries, own, pieces, slot, block, heads, place, scale):
    parts = len(pieces)
    tokens, size = sum(query.shape[1] for query in queries), own.shape[1]
    rows = own.shape[0]
    return pl.pallas_call(
        functools.partial(read_kernel, parts, scale),
        grid_spec=pltpu.PrefetchScalarGridSpec(
            num_scalar_prefetch=2,
            grid=(1,),
            in_specs=[pl.BlockSpec((2 * heads, size), lambda i, b, p: (rows // (2 * heads) - 1, 0))]
            + [pl.BlockSpec((1, rows, size), lambda i, b, p: (slot, 0, 0))] * parts
            + [
                pl.BlockSpec((1, query.shape[1], heads, size), lambda i, b, p: (0, 0, b[0], 0))
                for query in queries
            ],
            out_specs=pl.BlockSpec((tokens, heads * size), lambda i, b, p: (0, 0)),
            scratch_shapes=[
                pltpu.VMEM((tokens * heads, size), F32),
                pltpu.VMEM((heads * size, size), BF16),
            ],
        ),
        out_shape=jax.ShapeDtypeStruct((tokens, heads * size), BF16),
        cost_estimate=cost(heads * tokens * size * size * 8, heads * tokens * size * 4),
        compiler_params=pltpu.CompilerParams(vmem_limit_bytes=12 * MIB),
        name="read_states",
    )(block, place, own, *pieces, *queries)


def hold_kernel(weight, out, sem):
    copy = pltpu.make_async_copy(weight, out, sem)
    copy.start()
    copy.wait()


def hold(weight):
    return pl.pallas_call(
        hold_kernel,
        in_specs=[pl.BlockSpec(memory_space=pl.ANY)],
        out_specs=pl.BlockSpec(memory_space=pltpu.VMEM),
        scratch_shapes=[pltpu.SemaphoreType.DMA],
        out_shape=jax.ShapeDtypeStruct(weight.shape, weight.dtype),
        compiler_params=pltpu.CompilerParams(vmem_limit_bytes=weight_bytes(weight) + MIB),
        name="hold",
    )(weight)


def finish_kernel(product, *refs):
    first, second, out = refs[-3:]
    half = first.shape[1]
    out[0, :, :half] = (product[:, :half] + first[...].astype(F32)).astype(BF16)
    out[0, :, half:] = (product[:, half:] + second[...].astype(F32)).astype(BF16)


def finish(result, product, first, second, shape, start):
    tokens, width = product.shape
    whole = pl.BlockSpec((tokens, width // 2), lambda i: (0, 0))
    given = [] if result is None else [result]
    return pl.pallas_call(
        finish_kernel,
        grid=(1,),
        in_specs=[pl.BlockSpec((tokens, width), lambda i: (0, 0))]
        + [pl.BlockSpec(memory_space=pl.ANY)] * len(given)
        + [whole, whole],
        out_specs=pl.BlockSpec((1, tokens, width), lambda i: (0, 0, start // width)),
        out_shape=jax.ShapeDtypeStruct(shape, BF16),
        input_output_aliases={1: 0} if given else {},
        compiler_params=pltpu.CompilerParams(vmem_limit_bytes=24 * MIB),
        name="finish",
    )(product, *given, first, second)


def partial_states_plain(key, value, table, here, place, blocks, heads, parts, grant, joined):
    _, _, _, size = key.shape
    outs = [[] for _ in range(parts)]
    for b in range(blocks):
        start = table[here[0] * blocks + b] * heads
        key_block = feature_map(lax.dynamic_slice_in_dim(key[0], start, heads, 1))
        value_block = lax.dynamic_slice_in_dim(value[0], start, heads, 1)
        state = jnp.einsum("thd,the->hde", key_block, value_block, preferred_element_type=F32)
        state = state.reshape(heads * size, size).astype(BF16)
        mass = split_mass(jnp.sum(key_block.astype(F32), axis=0))
        rows = heads * size // parts
        for j in range(parts):
            piece = lax.dynamic_slice_in_dim(state, lax.rem(place[0] + j, parts) * rows, rows, 0)
            outs[j].append(jnp.concatenate([piece, mass]))
    outs = [jnp.stack(out) for out in outs]
    return [jnp.stack(outs, axis=1)] if joined else outs


def total_states_plain(takes, heads, count):
    total = sum(take.astype(F32) for take in takes) / count
    rows = total.shape[1] - 2 * heads
    mass = total[:, rows : rows + heads] + total[:, rows + heads :]
    return [
        jnp.concatenate([total[b, :rows].astype(BF16), split_mass(mass[b])])
        for b in range(total.shape[0])
    ]


def read_states_plain(queries, own, pieces, slot, block, heads, place, scale):
    parts = len(pieces)
    query = jnp.concatenate(queries, axis=1)[0]
    tokens, _, size = query.shape
    query = lax.dynamic_slice_in_dim(query, block[0] * heads, heads, 1)
    mass = own[-2 * heads :].astype(F32)
    stack = jnp.stack([piece[slot, : -2 * heads] for piece in pieces])
    order = lax.rem(place[0] + parts - jnp.arange(parts), parts)
    state = stack[order].reshape(heads, size, size)
    feature = feature_map(query)
    top = jnp.einsum("thd,hde->the", feature, state, preferred_element_type=F32)
    bottom = jnp.einsum(
        "thd,hd->th",
        feature.astype(F32),
        mass[:heads] + mass[heads:],
        precision=lax.Precision.HIGHEST,
    )
    read = top / (bottom + 0.001)[..., None] * scale
    return read.astype(BF16).reshape(tokens, heads * size)


def layer(query_rows, key_rows, value_rows, out_weight):
    n, parts = lax.axis_size("dp"), lax.axis_size("sp")
    _, tokens, all_heads, size = query_rows.shape
    heads, width = all_heads // n, out_weight.shape[1]
    count = tokens * parts
    fits = heads % 8 == 0 and (heads * size) % (16 * parts) == 0
    make_partial = partial_states if fits else partial_states_plain
    make_total = total_states if fits else total_states_plain
    make_read = read_states if fits else read_states_plain

    ring = ring_order(n)
    to = [[ring[(ring.index(d) + o) % n] for o in range(n)] for d in range(n)]
    here = lax.axis_index("dp").reshape(1)
    place = lax.axis_index("sp").reshape(1)

    def block_of(offset):
        found = jnp.int32(to[0][offset])
        for d in range(1, n):
            found = jnp.where(here[0] == d, to[d][offset], found)
        return found

    def around(x, offset):
        return lax.ppermute(x, "dp", [(d, to[d][offset % n]) for d in range(n)])

    def along(x, offset):
        return lax.ppermute(x, "sp", [(i, (i + offset) % parts) for i in range(parts)])

    groups = [g for g in (sorted({1, n - 1} - {n, 0}), list(range(2, n - 1)), [0]) if g]

    takes, queries, mixed = [], {}, {}
    for g, group in enumerate(groups):
        table = jnp.array([to[d][o] for d in range(n) for o in group], jnp.int32)
        size_of = (len(group), heads, parts, 16 if g else 56)
        far = g > 0 and group[0] > 0
        sent = make_partial(key_rows, value_rows, table, here, place, *size_of, far)
        if far:
            moved = [around(sent[0][i], o) for i, o in enumerate(group)]
            sent = [jnp.stack([x[j] for x in moved]) for j in range(parts)]
        takes.append([sent[0]] + [along(sent[j], j) for j in range(1, parts)])
        halves = [tokens // 4] if far else 1
        for o in group:
            if o:
                piece = lax.dynamic_slice_in_dim(query_rows, block_of(o) * heads, heads, 2)
                cuts = jnp.split(piece, halves, axis=1)
                for c, cut in enumerate(cuts):
                    cuts[c] = around(cut, o)
                queries[-o % n] = cuts
    for g, (group, take) in enumerate(zip(groups, takes)):
        owns = list(make_total(take, heads, count))
        if g == 0:
            owns = [around(own, o) if o else own for own, o in zip(owns, group)]
        stack = jnp.stack(owns) if len(owns) > 1 else owns[0][None]
        pieces = [stack] + [along(stack, j) for j in range(1, parts)]
        for i, o in enumerate(group):
            slot = -o % n
            query, block = (queries[slot], jnp.zeros(1, jnp.int32)) if o else ([query_rows], here)
            mixed[slot] = make_read(
                query, owns[i], pieces, i, block, heads, place, count**0.5
            )

    if fits and weight_bytes(out_weight) <= 16 * MIB:
        out_weight = hold(out_weight)

    lanes = []
    start, unit = 0, width // (2 * sum(SHARES))
    for share in SHARES:
        for way in (1, -1):
            lanes.append((way, out_weight[:, start : start + share * unit]))
            start += share * unit
    accs = []
    for way, weight in lanes:
        acc = jnp.dot(mixed[-way % n], weight, preferred_element_type=F32).astype(BF16)
        accs.append(acc)
    for k in range(1, n):
        for lane, (way, weight) in enumerate(lanes):
            accs[lane] = around(accs[lane], way)
            if k < n - 1:
                product = jnp.dot(mixed[-way * (k + 1) % n], weight, preferred_element_type=F32)
                accs[lane] = (product + accs[lane].astype(F32)).astype(BF16)
    result, start = None, 0
    for lane in range(0, len(lanes), 2):
        stop = start + 2 * lanes[lane][1].shape[1]
        weight = out_weight[:, start:stop]
        product = jnp.dot(mixed[0], weight, preferred_element_type=F32)
        pair = accs[lane : lane + 2]
        if fits:
            result = finish(result, product, *pair, (1, tokens, width), start)
        else:
            part = (product + jnp.concatenate(pair, axis=1).astype(F32)).astype(BF16)[None]
            result = part if result is None else jnp.concatenate([result, part], axis=2)
        start = stop
    return result


def solution(mesh):
    rows = P(("shift", "dp"), "sp", None, None)
    return jax.shard_map(
        layer,
        mesh=mesh,
        in_specs=(rows, rows, rows, P(("shift", "dp"), None)),
        out_specs=P(("shift", "dp"), "sp", None),
        check_vma=False,
    )
```

```python
import functools
import math

import jax
import jax.numpy as jnp
from jax import lax
from jax.experimental import pallas as pl
from jax.experimental.pallas import tpu as pltpu
from jax.sharding import PartitionSpec as P


F32, BF16 = jnp.float32, jnp.bfloat16
SHARES = (1, 1)
MIB = 1 << 20


def ring_order(n):
    side = math.isqrt(n)
    if side * side != n or side % 2:
        return list(range(n))
    order = list(range(side))
    for row in range(1, side):
        cols = range(1, side)
        order += [row * side + c for c in (reversed(cols) if row % 2 else cols)]
    order += [row * side for row in range(side - 1, 0, -1)]
    return order


def feature_map(values):
    wide = values.astype(F32)
    return jnp.where(wide > 0.0, wide + 1.0, jnp.exp(jnp.minimum(wide, 0.0))).astype(BF16)


def weight_bytes(weight):
    return weight.size * weight.dtype.itemsize


def cost(flops, nbytes):
    return pl.CostEstimate(flops=flops, bytes_accessed=nbytes, transcendentals=0)


def split_mass(mass):
    high = mass.astype(BF16)
    low = (mass - high.astype(F32)).astype(BF16)
    return jnp.concatenate([high, low], axis=0)


def state_kernel(parts, table, here, place, key, value, *refs):
    outs, (keys, values, states) = refs[:-3], refs[-3:]
    tokens, heads, size = key.shape[1:]
    rows = heads * size // parts
    feature = feature_map(key[0]).astype(F32)
    mass = split_mass(jnp.sum(feature, axis=0))
    keys[...] = feature.reshape(tokens * heads, size)
    values[...] = value[0].astype(F32).reshape(tokens * heads, size)
    for h in range(heads):
        states[h * size : (h + 1) * size, :] = lax.dot_general(
            keys[pl.ds(h, tokens, stride=heads), :].astype(BF16),
            values[pl.ds(h, tokens, stride=heads), :].astype(BF16),
            (((0,), (0,)), ((), ())),
            preferred_element_type=F32,
        )
    for j in range(parts):
        start = pl.multiple_of(lax.rem(place[0] + j, parts) * rows, rows)
        out = outs[j].at[0] if len(outs) == parts else outs[0].at[0, j]
        out[:rows, :] = states[pl.ds(start, rows), :].astype(BF16)
        out[rows:, :] = mass


def partial_states(key, value, table, here, place, blocks, heads, parts, grant, joined):
    _, tokens, _, size = key.shape
    rows = heads * size // parts + 2 * heads
    if joined:
        outs = [jax.ShapeDtypeStruct((blocks, parts, rows, size), BF16)]
        out_specs = [pl.BlockSpec((1, parts, rows, size), lambda i, t, d, p: (i, 0, 0, 0))]
    else:
        outs = [jax.ShapeDtypeStruct((blocks, rows, size), BF16)] * parts
        out_specs = [pl.BlockSpec((1, rows, size), lambda i, t, d, p: (i, 0, 0))] * parts
    block = pl.BlockSpec((1, tokens, heads, size), lambda i, t, d, p: (0, 0, t[d[0] * blocks + i], 0))
    return pl.pallas_call(
        functools.partial(state_kernel, parts),
        grid_spec=pltpu.PrefetchScalarGridSpec(
            num_scalar_prefetch=3,
            grid=(blocks,),
            in_specs=[block, block],
            out_specs=out_specs,
            scratch_shapes=[
                pltpu.VMEM((tokens * heads, size), F32),
                pltpu.VMEM((tokens * heads, size), F32),
                pltpu.VMEM((heads * size, size), F32),
            ],
        ),
        out_shape=outs,
        cost_estimate=cost(blocks * heads * tokens * size * size * 2, blocks * heads * tokens * size * 4),
        compiler_params=pltpu.CompilerParams(vmem_limit_bytes=grant * MIB),
        name="partial_states",
    )(table, here, place, key, value)


def total_kernel(blocks, heads, count, *refs):
    takes, outs = refs[:-blocks], refs[-blocks:]
    rows = takes[0].shape[1] - 2 * heads
    for b in range(blocks):
        total = takes[0][b].astype(F32)
        for take in takes[1:]:
            total = total + take[b].astype(F32)
        total = total / count
        outs[b][:rows, :] = total[:rows].astype(BF16)
        mass = total[rows : rows + heads] + total[rows + heads :]
        outs[b][rows:, :] = split_mass(mass)


def total_states(takes, heads, count):
    blocks, rows, size = takes[0].shape
    return pl.pallas_call(
        functools.partial(total_kernel, blocks, heads, count),
        out_shape=[jax.ShapeDtypeStruct((rows, size), BF16)] * blocks,
        cost_estimate=cost(blocks * rows * size * 8, blocks * rows * size * 10),
        compiler_params=pltpu.CompilerParams(vmem_limit_bytes=8 * MIB),
        name="total_states",
    )(*takes)


def read_kernel(parts, scale, block, place, mass, *refs):
    pieces, asked, (out, queries, states) = refs[:parts], refs[parts:-3], refs[-3:]
    heads, size = asked[0].shape[2:]
    tokens = out.shape[0]
    rows = heads * size // parts
    for j in range(parts):
        start = pl.multiple_of(lax.rem(place[0] + parts - j, parts) * rows, rows)
        states[pl.ds(start, rows), :] = pieces[j][0, :rows, :]
    done = 0
    for query in asked:
        some = query.shape[1] * heads
        queries[done : done + some, :] = feature_map(query[0]).astype(F32).reshape(some, size)
        done += some
    masses = mass[...].astype(F32)
    masses = (masses[:heads] + masses[heads:]).T
    none = jnp.zeros((size, size), BF16)
    for h in range(heads):
        feature = queries[pl.ds(h, tokens, stride=heads), :].astype(BF16)
        whole = jnp.broadcast_to(masses[:, h : h + 1], (size, size))
        high = whole.astype(BF16)
        low = (whole - high.astype(F32)).astype(BF16)
        state = jnp.concatenate([states[h * size : (h + 1) * size, :], none], axis=0)
        both = jnp.concatenate([state, jnp.concatenate([high, low], axis=0)], axis=1)
        read = jnp.dot(
            jnp.concatenate([feature, feature], axis=1), both, preferred_element_type=F32
        )
        result = read[:, :size] / (read[:, size:] + 0.001) * scale
        out[:, h * size : (h + 1) * size] = result.astype(BF16)


def read_states(queries, own, pieces, slot, block, heads, place, scale):
    parts = len(pieces)
    tokens, size = sum(query.shape[1] for query in queries), own.shape[1]
    rows = own.shape[0]
    return pl.pallas_call(
        functools.partial(read_kernel, parts, scale),
        grid_spec=pltpu.PrefetchScalarGridSpec(
            num_scalar_prefetch=2,
            grid=(1,),
            in_specs=[pl.BlockSpec((2 * heads, size), lambda i, b, p: (rows // (2 * heads) - 1, 0))]
            + [pl.BlockSpec((1, pieces[0].shape[1], size), lambda i, b, p: (slot, 0, 0))] * parts
            + [
                pl.BlockSpec((1, query.shape[1], heads, size), lambda i, b, p: (0, 0, b[0], 0))
                for query in queries
            ],
            out_specs=pl.BlockSpec((tokens, heads * size), lambda i, b, p: (0, 0)),
            scratch_shapes=[
                pltpu.VMEM((tokens * heads, size), F32),
                pltpu.VMEM((heads * size, size), BF16),
            ],
        ),
        out_shape=jax.ShapeDtypeStruct((tokens, heads * size), BF16),
        cost_estimate=cost(heads * tokens * size * size * 8, heads * tokens * size * 4),
        compiler_params=pltpu.CompilerParams(vmem_limit_bytes=12 * MIB),
        name="read_states",
    )(block, place, own, *pieces, *queries)


def hold_kernel(weight, out, sem):
    copy = pltpu.make_async_copy(weight, out, sem)
    copy.start()
    copy.wait()


def hold(weight):
    return pl.pallas_call(
        hold_kernel,
        in_specs=[pl.BlockSpec(memory_space=pl.ANY)],
        out_specs=pl.BlockSpec(memory_space=pltpu.VMEM),
        scratch_shapes=[pltpu.SemaphoreType.DMA],
        out_shape=jax.ShapeDtypeStruct(weight.shape, weight.dtype),
        compiler_params=pltpu.CompilerParams(vmem_limit_bytes=weight_bytes(weight) + MIB),
        name="hold",
    )(weight)


def finish_kernel(product, *refs):
    first, second, out = refs[-3:]
    half = first.shape[1]
    out[0, :, :half] = (product[:, :half] + first[...].astype(F32)).astype(BF16)
    out[0, :, half:] = (product[:, half:] + second[...].astype(F32)).astype(BF16)


def finish(result, product, first, second, shape, start):
    tokens, width = product.shape
    whole = pl.BlockSpec((tokens, width // 2), lambda i: (0, 0))
    given = [] if result is None else [result]
    return pl.pallas_call(
        finish_kernel,
        grid=(1,),
        in_specs=[pl.BlockSpec((tokens, width), lambda i: (0, 0))]
        + [pl.BlockSpec(memory_space=pl.ANY)] * len(given)
        + [whole, whole],
        out_specs=pl.BlockSpec((1, tokens, width), lambda i: (0, 0, start // width)),
        out_shape=jax.ShapeDtypeStruct(shape, BF16),
        input_output_aliases={1: 0} if given else {},
        compiler_params=pltpu.CompilerParams(vmem_limit_bytes=24 * MIB),
        name="finish",
    )(product, *given, first, second)


def partial_states_plain(key, value, table, here, place, blocks, heads, parts, grant, joined):
    _, _, _, size = key.shape
    outs = [[] for _ in range(parts)]
    for b in range(blocks):
        start = table[here[0] * blocks + b] * heads
        key_block = feature_map(lax.dynamic_slice_in_dim(key[0], start, heads, 1))
        value_block = lax.dynamic_slice_in_dim(value[0], start, heads, 1)
        state = jnp.einsum("thd,the->hde", key_block, value_block, preferred_element_type=F32)
        state = state.reshape(heads * size, size).astype(BF16)
        mass = split_mass(jnp.sum(key_block.astype(F32), axis=0))
        rows = heads * size // parts
        for j in range(parts):
            piece = lax.dynamic_slice_in_dim(state, lax.rem(place[0] + j, parts) * rows, rows, 0)
            outs[j].append(jnp.concatenate([piece, mass]))
    outs = [jnp.stack(out) for out in outs]
    return [jnp.stack(outs, axis=1)] if joined else outs


def total_states_plain(takes, heads, count):
    total = sum(take.astype(F32) for take in takes) / count
    rows = total.shape[1] - 2 * heads
    mass = total[:, rows : rows + heads] + total[:, rows + heads :]
    return [
        jnp.concatenate([total[b, :rows].astype(BF16), split_mass(mass[b])])
        for b in range(total.shape[0])
    ]


def read_states_plain(queries, own, pieces, slot, block, heads, place, scale):
    parts = len(pieces)
    query = jnp.concatenate(queries, axis=1)[0]
    tokens, _, size = query.shape
    query = lax.dynamic_slice_in_dim(query, block[0] * heads, heads, 1)
    mass = own[-2 * heads :].astype(F32)
    stack = jnp.stack([piece[slot, : heads * size // parts] for piece in pieces])
    order = lax.rem(place[0] + parts - jnp.arange(parts), parts)
    state = stack[order].reshape(heads, size, size)
    feature = feature_map(query)
    top = jnp.einsum("thd,hde->the", feature, state, preferred_element_type=F32)
    bottom = jnp.einsum(
        "thd,hd->th",
        feature.astype(F32),
        mass[:heads] + mass[heads:],
        precision=lax.Precision.HIGHEST,
    )
    read = top / (bottom + 0.001)[..., None] * scale
    return read.astype(BF16).reshape(tokens, heads * size)


def layer(query_rows, key_rows, value_rows, out_weight):
    n, parts = lax.axis_size("dp"), lax.axis_size("sp")
    _, tokens, all_heads, size = query_rows.shape
    heads, width = all_heads // n, out_weight.shape[1]
    count = tokens * parts
    fits = heads % 8 == 0 and (heads * size) % (16 * parts) == 0
    make_partial = partial_states if fits else partial_states_plain
    make_total = total_states if fits else total_states_plain
    make_read = read_states if fits else read_states_plain

    ring = ring_order(n)
    to = [[ring[(ring.index(d) + o) % n] for o in range(n)] for d in range(n)]
    here = lax.axis_index("dp").reshape(1)
    place = lax.axis_index("sp").reshape(1)

    def block_of(offset):
        found = jnp.int32(to[0][offset])
        for d in range(1, n):
            found = jnp.where(here[0] == d, to[d][offset], found)
        return found

    def around(x, offset):
        return lax.ppermute(x, "dp", [(d, to[d][offset % n]) for d in range(n)])

    def along(x, offset):
        return lax.ppermute(x, "sp", [(i, (i + offset) % parts) for i in range(parts)])

    groups = [g for g in (sorted({1, n - 1} - {n, 0}), list(range(2, n - 1)), [0]) if g]

    takes, queries, mixed = [], {}, {}
    for g, group in enumerate(groups):
        table = jnp.array([to[d][o] for d in range(n) for o in group], jnp.int32)
        size_of = (len(group), heads, parts, 16 if g else 56)
        far = g > 0 and group[0] > 0
        sent = make_partial(key_rows, value_rows, table, here, place, *size_of, far)
        if far:
            moved = [around(sent[0][i], o) for i, o in enumerate(group)]
            sent = [jnp.stack([x[j] for x in moved]) for j in range(parts)]
        takes.append([sent[0]] + [along(sent[j], j) for j in range(1, parts)])
        halves = [tokens // 4] if far else 1
        for o in group:
            if o:
                piece = lax.dynamic_slice_in_dim(query_rows, block_of(o) * heads, heads, 2)
                cuts = jnp.split(piece, halves, axis=1)
                for c, cut in enumerate(cuts):
                    cuts[c] = around(cut, o)
                queries[-o % n] = cuts
    for g, (group, take) in enumerate(zip(groups, takes)):
        owns = list(make_total(take, heads, count))
        if g == 0:
            owns = [around(own, o) if o else own for own, o in zip(owns, group)]
        stack = jnp.stack([own[: -2 * heads] for own in owns]) if group[0] else owns[0][None]
        pieces = [stack] + [along(stack, j) for j in range(1, parts)]
        for i, o in enumerate(group):
            slot = -o % n
            query, block = (queries[slot], jnp.zeros(1, jnp.int32)) if o else ([query_rows], here)
            mixed[slot] = make_read(
                query, owns[i], pieces, i, block, heads, place, count**0.5
            )

    if fits and weight_bytes(out_weight) <= 16 * MIB:
        out_weight = hold(out_weight)

    lanes = []
    start, unit = 0, width // (2 * sum(SHARES))
    for share in SHARES:
        for way in (1, -1):
            lanes.append((way, out_weight[:, start : start + share * unit]))
            start += share * unit
    accs = []
    for way, weight in lanes:
        acc = jnp.dot(mixed[-way % n], weight, preferred_element_type=F32).astype(BF16)
        accs.append(acc)
    for k in range(1, n):
        for lane, (way, weight) in enumerate(lanes):
            accs[lane] = around(accs[lane], way)
            if k < n - 1:
                product = jnp.dot(mixed[-way * (k + 1) % n], weight, preferred_element_type=F32)
                accs[lane] = (product + accs[lane].astype(F32)).astype(BF16)
    result, start = None, 0
    for lane in range(0, len(lanes), 2):
        stop = start + 2 * lanes[lane][1].shape[1]
        weight = out_weight[:, start:stop]
        product = jnp.dot(mixed[0], weight, preferred_element_type=F32)
        pair = accs[lane : lane + 2]
        if fits:
            result = finish(result, product, *pair, (1, tokens, width), start)
        else:
            part = (product + jnp.concatenate(pair, axis=1).astype(F32)).astype(BF16)[None]
            result = part if result is None else jnp.concatenate([result, part], axis=2)
        start = stop
    return result


def solution(mesh):
    rows = P(("shift", "dp"), "sp", None, None)
    return jax.shard_map(
        layer,
        mesh=mesh,
        in_specs=(rows, rows, rows, P(("shift", "dp"), None)),
        out_specs=P(("shift", "dp"), "sp", None),
        check_vma=False,
    )
```
